512 devices in a mesh: tm: 256 (over x, z_hi, y, core), space: 2 (over z_lo).
Axes of the slice: x: 4, y: 8, z: 8 (z_hi: 4, z_lo: 2; z = z_hi * 2 + z_lo), core: 2. Of those that a mesh axis runs over, the one named last changes fastest.
Arguments:
- initial: float32 [256, 32, 64, 128], P('tm', 'space'), may hold values from -6 to 6
- source: float32 [256, 32, 64, 128], P('tm', 'space'), may hold values from -6 to 6
- diffusion: float32 [32, 64, 128], P('space'), may hold values from 0.1 to 1
- advection: float32 [3, 32, 64, 128], P(None, 'space'), may hold values from 0.05 to 0.5
Outputs:
- smoothed: float32 [256, 32, 64, 128], P('tm', 'space')
- residual: float32 [256, 32, 64, 128], P('tm', 'space')
The draws below stay inside these ranges and needn't reach their ends.
All inputs are finite; a program needn't handle non-finite values.
Results may differ from the reference program's by a relative error of at most 0.00002.
Values sent between devices are 32-bit elements; how exact they have to be, the bound alone decides.
No kernel may reach another device: no remote copies, remote signals or barrier semaphores. Data moves between devices by JAX's collectives and lax.ppermute only.
A program may use at most 64 MiB of HBM per device.

```python
import math
import jax
import jax.numpy as jnp

SWEEPS = 2
ITERS = 4
NX = 64
NY = 128
NT = 256
NZ = 32


def level_of(stream_key, dims, pieces, smallest, top_value):
    def one(position, shards_of):
        draws = jax.random.uniform(jax.random.fold_in(jax.random.fold_in(stream_key, 6), position), (shards_of,), jnp.float32, smallest / len(pieces), top_value / len(pieces))
        return jnp.repeat(jnp.exp(draws), dims[position] // shards_of).reshape((-1,) + (1,) * (len(dims) - position - 1))

    level = one(*pieces[0])
    for cut in pieces[1:]:
        level = level * one(*cut)
    return level


def normal_values(own_key, shape, deviation, most, shards=(), kind=jnp.bfloat16):
    drawn = jax.random.normal(own_key, shape, jnp.float32) * deviation
    if len(shards) > 0:
        drawn = level_of(own_key, shape, shards, -0.22, 0.18) * drawn
    return jnp.clip(drawn, min=-most, max=most).astype(kind)


def setup_inputs(seed: int = 0) -> dict:
    seeds = jax.random.split(jax.random.key(seed), 5)
    initial = normal_values(seeds[0], (NT, NZ, NX, NY), 1.0, 6.0, ((0, 256), (1, 2)), jnp.float32)
    source = normal_values(seeds[1], (NT, NZ, NX, NY), 1.0, 6.0, ((0, 256), (1, 2)), jnp.float32)
    diffusion = jnp.clip(jnp.exp(math.log(1.0) - 2.3025851 * jax.random.uniform(seeds[2], (NZ, NX, NY), jnp.float32) ** level_of(seeds[2], (NZ, NX, NY), ((0, 2),), -0.2, 0.2)), 0.1, 1.0)
    advection = jnp.clip(jnp.exp(math.log(0.5) - 2.3025851 * jax.random.uniform(seeds[3], (3, NZ, NX, NY), jnp.float32) ** level_of(seeds[3], (3, NZ, NX, NY), ((1, 2),), -0.2, 0.2)), 0.05, 0.5)
    return {"initial": initial, "source": source, "diffusion": diffusion, "advection": advection}


def off_terms(padded, spread, upwind):
    low_z = padded[..., :-2, 1:-1, 1:-1]
    high_z = padded[..., 2:, 1:-1, 1:-1]
    low_x = padded[..., 1:-1, :-2, 1:-1]
    high_x = padded[..., 1:-1, 2:, 1:-1]
    low_y = padded[..., 1:-1, 1:-1, :-2]
    high_y = padded[..., 1:-1, 1:-1, 2:]
    total = spread * (high_z + low_z + high_x + low_x + high_y + low_y)
    return total + upwind[0] * low_x + upwind[1] * low_y + upwind[2] * low_z


def main_diagonal(spread, upwind):
    return 1.0 + 6.0 * spread + (upwind[0] + upwind[1] + upwind[2])


def pad_space(field):
    return jnp.pad(field, ((0, 0), (1, 1), (1, 1), (1, 1)))


def reference(initial, source, diffusion, advection):
    diagonal = main_diagonal(diffusion, advection)
    smoothed = initial
    for sweep in range(SWEEPS):
        prior = jnp.roll(smoothed, 1, axis=0)
        forcing = prior + source
        current = smoothed
        for step in range(ITERS):
            current = (forcing + off_terms(pad_space(current), diffusion, advection)) / diagonal
        smoothed = current
    prior = jnp.roll(smoothed, 1, axis=0)
    applied = diagonal * smoothed - off_terms(pad_space(smoothed), diffusion, advection)
    residual = source + prior - applied
    return smoothed, residual
```

```python
import jax
import jax.numpy as jnp
from jax import lax
from jax.experimental import pallas as pl
from jax.experimental.pallas import tpu as pltpu
from jax.sharding import PartitionSpec as P

SWEEPS = 2
ITERS = 4
THIN = ITERS - 1
F32 = jnp.float32
ROLE, SIDE = 0, 1


def in_vmem(count):
    return [pl.BlockSpec(memory_space=pltpu.VMEM)] * count


def call(kernel, outs, scalars, *operands, scratch=()):
    return pl.pallas_call(
        kernel,
        out_shape=[jax.ShapeDtypeStruct(o, F32) for o in outs],
        in_specs=[pl.BlockSpec(memory_space=pltpu.SMEM)] + in_vmem(len(operands)),
        out_specs=in_vmem(len(outs)),
        scratch_shapes=list(scratch),
        compiler_params=pltpu.CompilerParams(vmem_limit_bytes=16 * 1024 * 1024),
    )(scalars, *operands)


def coef_kernel(scal, spread_ref, upwind_ref, halo_ref, c_ref, x_ref, y_ref, z_ref, inv_ref, diag_ref):
    side = scal[SIDE]
    depth, nx, ny = spread_ref.shape
    row = lax.broadcasted_iota(jnp.int32, (nx, ny), 0)
    lane = lax.broadcasted_iota(jnp.int32, (nx, ny), 1)

    def one(spread, ux, uy, uz, at):
        diagonal = 1.0 + 6.0 * spread + (ux + uy + uz)
        inv = 1.0 / diagonal
        c_ref[at] = spread * inv
        x_ref[at] = jnp.where(row == 0, 0.0, (spread + ux) * inv)
        y_ref[at] = jnp.where(lane == 0, 0.0, (spread + uy) * inv)
        z_ref[at] = (spread + uz) * inv
        inv_ref[at] = inv
        return diagonal

    def own(z, carry):
        diag_ref[z] = one(spread_ref[z], upwind_ref[0, z], upwind_ref[1, z], upwind_ref[2, z], ITERS * side + z)
        return carry

    lax.fori_loop(0, depth, own, 0, unroll=2)
    for q in range(THIN):
        at = jnp.where(side == 1, 1 + q, depth + q)
        one(halo_ref[q], halo_ref[THIN + q], halo_ref[2 * THIN + q], halo_ref[3 * THIN + q], at)


def stencil(below, here, above, c, cx, cy, cz, row_last, lane_last):
    nx, ny = here.shape
    low_x = pltpu.roll(here, 1, 0)
    high_x = jnp.where(row_last, 0.0, pltpu.roll(here, nx - 1, 0))
    low_y = pltpu.roll(here, 1, 1)
    high_y = jnp.where(lane_last, 0.0, pltpu.roll(here, ny - 1, 1))
    return c * ((above + high_x) + high_y) + (cx * low_x + cz * below) + cy * low_y


def last_masks(nx, ny):
    row = lax.broadcasted_iota(jnp.int32, (nx, ny), 0)
    lane = lax.broadcasted_iota(jnp.int32, (nx, ny), 1)
    return row == nx - 1, lane == ny - 1


def sweep_kernel(role, pass_on, scal, *refs):
    if pass_on:
        other_ref, *refs = refs
    (v_ref, vh_ref, s_ref, sh_ref, p_ref, ph_ref, c_ref, x_ref, y_ref, z_ref, inv_ref, out_ref, edge4_ref, edge3_ref, va, vb, g) = refs
    side = scal[SIDE]
    depth, nx, ny = v_ref.shape

    @pl.when(scal[ROLE] == role)
    def _():
        row_last, lane_last = last_masks(nx, ny)
        zero = jnp.zeros((nx, ny), F32)
        for buf in (va, vb):
            buf[0] = zero
            buf[depth + ITERS + 1] = zero

        def fill(z, carry):
            at = ITERS * side + z
            va[1 + at] = v_ref[z]
            g[at] = (s_ref[z] + p_ref[z]) * inv_ref[at]
            return carry

        lax.fori_loop(0, depth, fill, 0, unroll=4)
        for q in range(ITERS):
            va[1 + jnp.where(side == 1, q, depth + q)] = vh_ref[q]
        for q in range(THIN):
            at = jnp.where(side == 1, 1 + q, depth + q)
            g[at] = (sh_ref[q] + ph_ref[q]) * inv_ref[at]
        src, dst = va, vb
        for k in range(ITERS):
            start = side * (1 + k)
            last = k == ITERS - 1

            def layer(j, carry, src=src, dst=dst, start=start, last=last):
                e = start + j
                new = g[e] + stencil(
                    src[e], src[e + 1], src[e + 2], c_ref[e], x_ref[e], y_ref[e], z_ref[e], row_last, lane_last
                )
                if last:
                    out_ref[j] = new
                else:
                    dst[e + 1] = new
                return carry

            count = depth + ITERS - 1 - k
            lax.fori_loop(0, count, layer, 0, unroll=True)
            src, dst = dst, src

    if pass_on:

        @pl.when(scal[ROLE] != role)
        def _():
            out_ref[...] = other_ref[...]

        for q in range(edge4_ref.shape[0]):
            edge4_ref[q] = out_ref[jnp.where(side == 1, q, depth - edge4_ref.shape[0] + q)]
    for q in range(THIN):
        edge3_ref[q] = out_ref[jnp.where(side == 1, q, depth - THIN + q)]


def defect_kernel(scal, v_ref, h_ref, s_ref, c_ref, x_ref, y_ref, z_ref, diag_ref, out_ref, va):
    side = scal[SIDE]
    depth, nx, ny = v_ref.shape
    row_last, lane_last = last_masks(nx, ny)
    zero = jnp.zeros((nx, ny), F32)
    va[0] = jnp.where(side == 1, h_ref[0], zero)
    va[depth + 1] = jnp.where(side == 1, zero, h_ref[0])
    for z in range(depth):
        va[1 + z] = v_ref[z]

    def layer(z, carry):
        e = ITERS * side + z
        here = va[1 + z]
        m = stencil(va[z], here, va[z + 2], c_ref[e], x_ref[e], y_ref[e], z_ref[e], row_last, lane_last)
        out_ref[z] = s_ref[z] - diag_ref[z] * (here - m)
        return carry

    lax.fori_loop(0, depth, layer, 0, unroll=True)


def body(initial, source, diffusion, advection):
    tm, space = (lax.axis_size("tm"), lax.axis_size("space"))
    role = lax.axis_index("tm") % 2
    side = lax.axis_index("space")
    scalars = jnp.stack([role, side]).astype(jnp.int32)
    shape = initial.shape[1:]
    depth = shape[0]
    initial, source = (initial[0], source[0])

    def number(t, s):
        return (t % tm) * space + s

    def permute(value, pairs):
        return lax.ppermute(value, ("tm", "space"), pairs)

    sides = range(space)
    into_odd = [(number(t, s), number(t + 1, s)) for t in range(0, tm, 2) for s in sides]
    into_even = [(number(t, s), number(t + 1, s)) for t in range(1, tm, 2) for s in sides]
    across = [(number(t, s), number(t, 1 - s)) for t in range(tm) for s in sides]
    odd_across = [(number(t, s), number(t + 1, 1 - s)) for t in range(0, tm, 2) for s in sides]
    even_across = [(number(t, s), number(t + 1, 1 - s)) for t in range(1, tm, 2) for s in sides]

    def edge(value, width, axis=0):
        return lax.dynamic_slice_in_dim(value, (1 - side) * (depth - width), width, axis)

    ext = (depth + ITERS,) + shape[1:]
    padded = (depth + ITERS + 2,) + shape[1:]
    scratch = [pltpu.VMEM(padded, F32), pltpu.VMEM(padded, F32), pltpu.VMEM(ext, F32)]
    thin = (THIN,) + shape[1:]
    wide = (ITERS,) + shape[1:]

    b1 = permute(initial, into_even)
    d1 = permute(edge(initial, THIN), odd_across + even_across)
    halo = jnp.concatenate(
        [edge(diffusion, THIN), edge(advection, THIN, 1).reshape((3 * THIN,) + shape[1:]), edge(source, THIN), edge(initial, ITERS)], 0
    )
    halo = permute(halo, across)
    a1 = permute(initial, into_odd)
    *coefs, diag = call(coef_kernel, [ext] * 5 + [shape], scalars, diffusion, advection, halo)
    source_halo = halo[4 * THIN : 5 * THIN]
    initial_halo = halo[5 * THIN :]

    def sweep(mine, other, v, vh, p, ph):
        import functools

        outs = [shape, wide if mine == 0 else (1,) + shape[1:], thin]
        pass_on = other is not None
        extra = [other] if pass_on else []
        return call(
            functools.partial(sweep_kernel, mine, pass_on), outs, scalars, *extra, v, vh, source, source_halo, p, ph, *coefs, scratch=scratch
        )

    x, _, xt = sweep(1, None, initial, initial_halo, a1, d1)
    b2 = permute(x, into_even)
    dx = permute(xt, even_across)
    s1, s1w, s1t = sweep(0, x, initial, initial_halo, b1, d1)
    dy = permute(s1t, odd_across)
    s1h = permute(s1w, across)
    a2 = permute(s1, into_odd)
    z, _, _ = sweep(1, None, s1, s1h, a2, dy)
    b3 = permute(z, into_even)
    s2, s2w, _ = sweep(0, z, s1, s1h, b2, dx)
    a3 = permute(s2, into_odd)
    side_edge = edge(s2, 1)
    s2h = permute(side_edge, across)
    (defect,) = call(defect_kernel, [shape], scalars, s2, s2h, source, *coefs[:4], diag, scratch=[pltpu.VMEM((depth + 2,) + shape[1:], F32)])
    residual = defect + (a3 + b3)
    return (s2[None], residual[None])


def solution(mesh):
    in_specs = (
        P("tm", "space", None, None),
        P("tm", "space", None, None),
        P("space", None, None),
        P(None, "space", None, None),
    )
    out_specs = (P("tm", "space", None, None), P("tm", "space", None, None))
    return jax.shard_map(body, mesh=mesh, in_specs=in_specs, out_specs=out_specs, check_vma=False)
```

```python
import functools

import jax
import jax.numpy as jnp
from jax import lax
from jax.experimental import pallas as pl
from jax.experimental.pallas import tpu as pltpu
from jax.sharding import PartitionSpec as P


ITERS = 4
THIN = ITERS - 1
F32 = jnp.float32
ROLE, SIDE = 0, 1
ROW, RUNS = 16, 4


def call(kernel, outs, scalars, *operands, far=(), scratch=(), aliases=None):
    far = [pltpu.with_memory_space_constraint(o, pltpu.HBM) for o in far]
    near = [pltpu.with_memory_space_constraint(o, pltpu.VMEM) for o in operands]
    return pl.pallas_call(
        kernel,
        out_shape=[o if not isinstance(o, tuple) else pltpu.VMEM(o, F32) for o in outs],
        in_specs=[pl.BlockSpec(memory_space=pltpu.SMEM)]
        + [pl.BlockSpec(memory_space=pltpu.HBM)] * len(far)
        + [pl.BlockSpec(memory_space=pltpu.VMEM)] * len(near),
        out_specs=[pl.BlockSpec(memory_space=pltpu.VMEM if isinstance(o, tuple) else pltpu.HBM) for o in outs],
        scratch_shapes=list(scratch),
        input_output_aliases=aliases or {},
        compiler_params=pltpu.CompilerParams(vmem_limit_bytes=16 * 1024 * 1024),
    )(scalars, *far, *near)


def pack_kernel(scal, init_ref, source_ref, spread_ref, upwind_ref, coef_out, field_out, thin_out, sem):
    side = scal[SIDE]
    depth = init_ref.shape[0]
    thin = pl.ds((1 - side) * (depth - THIN), THIN)
    wide = pl.ds((1 - side) * (depth - ITERS), ITERS)
    copies = [
        pltpu.make_async_copy(init_ref.at[wide], field_out.at[pl.ds(0, ITERS)], sem.at[0]),
        pltpu.make_async_copy(source_ref.at[thin], field_out.at[pl.ds(ITERS, THIN)], sem.at[1]),
        pltpu.make_async_copy(init_ref.at[thin], thin_out, sem.at[6]),
        pltpu.make_async_copy(spread_ref.at[thin], coef_out.at[pl.ds(0, THIN)], sem.at[2]),
    ]
    for i in range(3):
        copies.append(pltpu.make_async_copy(upwind_ref.at[i, thin], coef_out.at[pl.ds((1 + i) * THIN, THIN)], sem.at[3 + i]))
    for copy in copies:
        copy.start()
    for copy in copies:
        copy.wait()


def weights(spread, ux, uy, uz, at, refs):
    c_ref, x_ref, y_ref, z_ref, inv_ref = refs
    nx, ny = spread.shape
    row = lax.broadcasted_iota(jnp.int32, (nx, ny), 0)
    lane = lax.broadcasted_iota(jnp.int32, (nx, ny), 1)
    diagonal = 1.0 + 6.0 * spread + (ux + uy + uz)
    inv = 1.0 / diagonal
    c_ref[at] = spread * inv
    x_ref[at] = jnp.where(row == 0, 0.0, (spread + ux) * inv)
    y_ref[at] = jnp.where(lane == 0, 0.0, (spread + uy) * inv)
    z_ref[at] = (spread + uz) * inv
    inv_ref[at] = inv
    return diagonal


def own_kernel(scal, init_far, source_far, spread_far, upwind_far, c_ref, x_ref, y_ref, z_ref, inv_ref, diag_ref, init_ref, source_ref, spread_ref, upwind_ref, sem):
    side = scal[SIDE]
    depth = init_far.shape[0]
    copies = [
        pltpu.make_async_copy(spread_far, spread_ref, sem.at[0]),
        pltpu.make_async_copy(upwind_far, upwind_ref, sem.at[1]),
        pltpu.make_async_copy(init_far, init_ref, sem.at[2]),
        pltpu.make_async_copy(source_far, source_ref, sem.at[3]),
    ]
    for copy in copies:
        copy.start()
    for copy in copies[:2]:
        copy.wait()

    def own(z, carry):
        diag_ref[z] = weights(
            spread_ref[z], upwind_ref[0, z], upwind_ref[1, z], upwind_ref[2, z], ITERS * side + z, (c_ref, x_ref, y_ref, z_ref, inv_ref)
        )
        return carry

    lax.fori_loop(0, depth, own, 0, unroll=2)
    for copy in copies[2:]:
        copy.wait()


def rim_kernel(scal, first_ref, second_ref, *refs):
    side = scal[SIDE]
    outs = refs[5:]
    depth = outs[0].shape[0] - ITERS
    for q in range(THIN):
        at = jnp.where(side == 1, 1 + q, depth + q)
        parts = [first_ref[i * THIN + q] + second_ref[i * THIN + q] for i in range(4)]
        weights(*parts, at, outs)


def stencil(below, here, above, c, cx, cy, cz, row_last, lane_last):
    nx, ny = here.shape
    low_x = pltpu.roll(here, 1, 0)
    high_x = jnp.where(row_last, 0.0, pltpu.roll(here, nx - 1, 0))
    low_y = pltpu.roll(here, 1, 1)
    high_y = jnp.where(lane_last, 0.0, pltpu.roll(here, ny - 1, 1))
    return c * ((above + high_x) + high_y) + (cx * low_x + cz * below) + cy * low_y


def last_masks(nx, ny):
    row = lax.broadcasted_iota(jnp.int32, (nx, ny), 0)
    lane = lax.broadcasted_iota(jnp.int32, (nx, ny), 1)
    return row == nx - 1, lane == ny - 1


def sweep_kernel(role, pass_on, widths, scal, *refs):
    if pass_on:
        other_ref, *refs = refs
    count = len(refs) - len(widths) - 3
    edge_refs = refs[count : count + len(widths)]
    refs = refs[:count] + refs[count + len(widths) :]
    (v_ref, vh_ref, s_ref, rim_ref, p_ref, ph_ref, c_ref, x_ref, y_ref, z_ref, inv_ref, out_ref, va, vb, g) = refs
    side = scal[SIDE]
    depth, nx, ny = v_ref.shape

    @pl.when(scal[ROLE] == role)
    def _():
        row_last, lane_last = last_masks(nx, ny)
        zero = jnp.zeros((nx, ny), F32)
        for buf in (va, vb):
            buf[0] = zero
            buf[depth + ITERS + 1] = zero

        def fill(z, carry):
            at = ITERS * side + z
            va[1 + at] = v_ref[z]
            g[at] = (s_ref[z] + p_ref[z]) * inv_ref[at]
            return carry

        lax.fori_loop(0, depth, fill, 0, unroll=4)
        for q in range(ITERS):
            va[1 + jnp.where(side == 1, q, depth + q)] = vh_ref[q]
        for q in range(THIN):
            at = jnp.where(side == 1, 1 + q, depth + q)
            g[at] = (rim_ref[ITERS + q] + ph_ref[q]) * inv_ref[at]
        src, dst = va, vb
        for k in range(ITERS):
            start = side * (1 + k)
            last = k == ITERS - 1

            def layer(j, carry, src=src, dst=dst, start=start, last=last):
                e = start + j
                new = g[e] + stencil(
                    src[e], src[e + 1], src[e + 2], c_ref[e], x_ref[e], y_ref[e], z_ref[e], row_last, lane_last
                )
                if last:
                    out_ref[j] = new
                else:
                    dst[e + 1] = new
                return carry

            count = depth + ITERS - 1 - k
            lax.fori_loop(0, count, layer, 0, unroll=True)
            src, dst = dst, src

    if pass_on:

        @pl.when(scal[ROLE] != role)
        def _():
            out_ref[...] = other_ref[...]

    for width, edge_ref in zip(widths, edge_refs):
        for q in range(width):
            edge_ref[q] = out_ref[jnp.where(side == 1, q, depth - width + q)]


def defect_kernel(scal, v_ref, h_ref, s_ref, c_ref, x_ref, y_ref, z_ref, diag_ref, out_ref, far_out, va, sem):
    side = scal[SIDE]
    depth, nx, ny = v_ref.shape
    copy = pltpu.make_async_copy(v_ref, far_out, sem)
    copy.start()
    row_last, lane_last = last_masks(nx, ny)
    zero = jnp.zeros((nx, ny), F32)
    va[0] = jnp.where(side == 1, h_ref[0], zero)
    va[depth + 1] = jnp.where(side == 1, zero, h_ref[0])
    for z in range(depth):
        va[1 + z] = v_ref[z]

    def layer(z, carry):
        e = ITERS * side + z
        here = va[1 + z]
        m = stencil(va[z], here, va[z + 2], c_ref[e], x_ref[e], y_ref[e], z_ref[e], row_last, lane_last)
        out_ref[z] = s_ref[z] - diag_ref[z] * (here - m)
        return carry

    lax.fori_loop(0, depth, layer, 0, unroll=True)
    copy.wait()


def add_kernel(scal, a_ref, b_ref, c_ref, far_out, out_ref, sem):
    pieces = sem.shape[0]
    size = out_ref.shape[0] // pieces
    copies = []
    for i in range(pieces):
        part = pl.ds(i * size, size)
        out_ref[part] = a_ref[part] + (b_ref[part] + c_ref[part])
        copies.append(pltpu.make_async_copy(out_ref.at[part], far_out.at[part], sem.at[i]))
        copies[-1].start()
    for copy in copies:
        copy.wait()


def body(initial, source, diffusion, advection):
    tm, space = (lax.axis_size("tm"), lax.axis_size("space"))
    role = lax.axis_index("tm") % 2
    side = lax.axis_index("space")
    scalars = jnp.stack([role, side]).astype(jnp.int32)
    shape = initial.shape[1:]
    depth = shape[0]
    initial, source = (initial[0], source[0])

    def number(t, s):
        return (t % tm) * space + s

    def permute(value, pairs):
        return lax.ppermute(value, ("tm", "space"), pairs)

    sides = range(space)
    stride, group = ROW, ROW * RUNS
    even, odd = range(0, tm, 2), range(1, tm, 2)
    into_odd = [(number(t, s), number(t + 1, s)) for t in even for s in sides]
    into_even = [(number(t, s), number(t + 1, s)) for t in odd for s in sides]
    across_even = [(number(t, s), number(t, 1 - s)) for t in even for s in sides]
    across_odd = [(number(t, s), number(t, 1 - s)) for t in odd for s in sides]
    odd_across = [(number(t, s), number(t + 1, 1 - s)) for t in even for s in sides]
    even_across = [(number(t, s), number(t + 1, 1 - s)) for t in odd for s in sides]
    lower_odd = [(number(t, 1), number(t, 0)) for t in odd]
    lower_odd += [(number(t, 0), number(t - stride if t % group >= stride else t - stride + group, 1)) for t in odd]
    back = [(number(t, s), number(t - 1, s)) for t in odd for s in sides]

    plane = shape[1:]
    ext = (depth + ITERS,) + plane
    padded = (depth + ITERS + 2,) + plane
    scratch = [pltpu.VMEM(padded, F32), pltpu.VMEM(padded, F32), pltpu.VMEM(ext, F32)]
    thin = (THIN,) + plane
    far = (initial, source, diffusion, advection)

    coef_edge, field_edge, thin_edge = call(
        pack_kernel, [(4 * THIN,) + plane, (ITERS + THIN,) + plane, thin], scalars, far=far, scratch=[pltpu.SemaphoreType.DMA((7,))]
    )
    sc = permute(coef_edge, lower_odd)
    b1 = permute(initial, into_even)
    rim = permute(field_edge, across_even + across_odd)
    d1 = permute(thin_edge, odd_across + even_across)
    a1 = permute(initial, into_odd)
    *coefs, diag, initial_near, source_near = call(
        own_kernel,
        [ext] * 5 + [shape] * 3,
        scalars,
        far=far,
        scratch=[pltpu.VMEM(shape, F32), pltpu.VMEM((3,) + shape, F32), pltpu.SemaphoreType.DMA((4,))],
    )
    ac = permute(sc, back)
    coefs = call(rim_kernel, [ext] * 5, scalars, sc, ac, *coefs, aliases={3 + i: i for i in range(5)})

    def sweep(mine, other, v, vh, p, ph, widths):
        outs = [shape] + [(w,) + plane for w in widths]
        extra = [other] if other is not None else []
        kernel = functools.partial(sweep_kernel, mine, other is not None, widths)
        return call(kernel, outs, scalars, *extra, v, vh, source_near, rim, p, ph, *coefs, scratch=scratch)

    x, xw, xt = sweep(1, None, initial_near, rim, a1, d1, (ITERS, THIN))
    b2 = permute(x, into_even)
    sx = permute(xw, across_odd)
    dx = permute(xt, even_across)
    s1, yw, yt = sweep(0, x, initial_near, rim, b1, d1, (ITERS, THIN))
    dy = permute(yt, odd_across)
    a2 = permute(s1, into_odd)
    sy = permute(yw, across_even)
    (z,) = sweep(1, None, s1, sx, a2, dy, ())
    b3 = permute(z, into_even)
    s2, s2w = sweep(0, z, s1, sy, b2, dx, (1,))
    a3 = permute(s2, into_odd)
    s2h = permute(s2w, across_even + across_odd)
    defect, s2_far = call(
        defect_kernel,
        [shape, pltpu.HBM(shape, F32)],
        scalars,
        s2,
        s2h,
        source_near,
        *coefs[:4],
        diag,
        scratch=[pltpu.VMEM((depth + 2,) + plane, F32), pltpu.SemaphoreType.DMA],
    )
    (residual,) = call(
        add_kernel, [pltpu.HBM(shape, F32)], scalars, defect, a3, b3, scratch=[pltpu.VMEM(shape, F32), pltpu.SemaphoreType.DMA((4,))]
    )
    return (s2_far[None], residual[None])


def solution(mesh):
    in_specs = (
        P("tm", "space", None, None),
        P("tm", "space", None, None),
        P("space", None, None),
        P(None, "space", None, None),
    )
    out_specs = (P("tm", "space", None, None), P("tm", "space", None, None))
    return jax.shard_map(body, mesh=mesh, in_specs=in_specs, out_specs=out_specs, check_vma=False)
```

```python
import functools

import jax
import jax.numpy as jnp
from jax import lax
from jax.experimental import pallas as pl
from jax.experimental.pallas import tpu as pltpu
from jax.sharding import PartitionSpec as P


ITERS = 4
THIN = ITERS - 1
F32 = jnp.float32
ROLE, SIDE = 0, 1
ROW, RUNS, CORES = 16, 4, 2
HELPER = 6


def call(kernel, outs, scalars, *operands, far=(), scratch=(), aliases=None):
    far = [pltpu.with_memory_space_constraint(o, pltpu.HBM) for o in far]
    near = [pltpu.with_memory_space_constraint(o, pltpu.VMEM) for o in operands]
    return pl.pallas_call(
        kernel,
        out_shape=[o if not isinstance(o, tuple) else pltpu.VMEM(o, F32) for o in outs],
        in_specs=[pl.BlockSpec(memory_space=pltpu.SMEM)]
        + [pl.BlockSpec(memory_space=pltpu.HBM)] * len(far)
        + [pl.BlockSpec(memory_space=pltpu.VMEM)] * len(near),
        out_specs=[pl.BlockSpec(memory_space=pltpu.VMEM if isinstance(o, tuple) else pltpu.HBM) for o in outs],
        scratch_shapes=list(scratch),
        input_output_aliases=aliases or {},
        compiler_params=pltpu.CompilerParams(vmem_limit_bytes=16 * 1024 * 1024),
    )(scalars, *far, *near)


def pack_kernel(scal, init_ref, source_ref, spread_ref, upwind_ref, coef_out, field_out, thin_out, sem):
    side = scal[SIDE]
    depth = init_ref.shape[0]
    thin = pl.ds((1 - side) * (depth - THIN), THIN)
    wide = pl.ds((1 - side) * (depth - ITERS), ITERS)
    copies = [
        pltpu.make_async_copy(init_ref.at[wide], field_out.at[pl.ds(0, ITERS)], sem.at[0]),
        pltpu.make_async_copy(source_ref.at[thin], field_out.at[pl.ds(ITERS, THIN)], sem.at[1]),
        pltpu.make_async_copy(init_ref.at[thin], thin_out, sem.at[6]),
        pltpu.make_async_copy(spread_ref.at[thin], coef_out.at[pl.ds(0, THIN)], sem.at[2]),
    ]
    for i in range(3):
        copies.append(pltpu.make_async_copy(upwind_ref.at[i, thin], coef_out.at[pl.ds((1 + i) * THIN, THIN)], sem.at[3 + i]))
    for copy in copies:
        copy.start()
    for copy in copies:
        copy.wait()


def weights(spread, ux, uy, uz, at, refs):
    c_ref, x_ref, y_ref, z_ref, inv_ref = refs
    nx, ny = spread.shape
    row = lax.broadcasted_iota(jnp.int32, (nx, ny), 0)
    lane = lax.broadcasted_iota(jnp.int32, (nx, ny), 1)
    diagonal = 1.0 + 6.0 * spread + (ux + uy + uz)
    inv = 1.0 / diagonal
    c_ref[at] = spread * inv
    x_ref[at] = jnp.where(row == 0, 0.0, (spread + ux) * inv)
    y_ref[at] = jnp.where(lane == 0, 0.0, (spread + uy) * inv)
    z_ref[at] = (spread + uz) * inv
    inv_ref[at] = inv
    return diagonal


def own_kernel(role, held, scal, init_far, source_far, spread_far, upwind_far, *refs):
    c_ref, x_ref, y_ref, z_ref, inv_ref, diag_ref, init_ref, source_ref, spread_ref, upwind_ref, sem = refs[held:]
    side = scal[SIDE]
    depth = init_far.shape[0]

    @pl.when(scal[ROLE] == role)
    def _():
        copies = [
            pltpu.make_async_copy(spread_far, spread_ref, sem.at[0]),
            pltpu.make_async_copy(upwind_far, upwind_ref, sem.at[1]),
            pltpu.make_async_copy(init_far, init_ref, sem.at[2]),
            pltpu.make_async_copy(source_far, source_ref, sem.at[3]),
        ]
        for copy in copies:
            copy.start()
        for copy in copies[:2]:
            copy.wait()

        def own(z, carry):
            diag_ref[z] = weights(
                spread_ref[z], upwind_ref[0, z], upwind_ref[1, z], upwind_ref[2, z], ITERS * side + z, (c_ref, x_ref, y_ref, z_ref, inv_ref)
            )
            return carry

        lax.fori_loop(0, depth, own, 0, unroll=2)
        for copy in copies[2:]:
            copy.wait()


def rim_kernel(count, scal, *refs):
    side = scal[SIDE]
    sources, outs = refs[:count], refs[count + 5 :]
    depth = outs[0].shape[0] - ITERS
    for q in range(THIN):
        at = jnp.where(side == 1, 1 + q, depth + q)
        parts = [sum(ref[i * THIN + q] for ref in sources) for i in range(4)]
        weights(*parts, at, outs)


def stencil(below, here, above, c, cx, cy, cz, row_last, lane_last):
    nx, ny = here.shape
    low_x = pltpu.roll(here, 1, 0)
    high_x = jnp.where(row_last, 0.0, pltpu.roll(here, nx - 1, 0))
    low_y = pltpu.roll(here, 1, 1)
    high_y = jnp.where(lane_last, 0.0, pltpu.roll(here, ny - 1, 1))
    return c * ((above + high_x) + high_y) + (cx * low_x + cz * below) + cy * low_y


def last_masks(nx, ny):
    row = lax.broadcasted_iota(jnp.int32, (nx, ny), 0)
    lane = lax.broadcasted_iota(jnp.int32, (nx, ny), 1)
    return row == nx - 1, lane == ny - 1


def sweep_kernel(role, pass_on, widths, halo_at, scal, *refs):
    if pass_on:
        other_ref, *refs = refs
    count = len(refs) - len(widths) - 3
    edge_refs = refs[count : count + len(widths)]
    refs = refs[:count] + refs[count + len(widths) :]
    v_ref, vh_ref, s_ref, rim_ref, p_ref, *ph_refs = refs[:-9]
    c_ref, x_ref, y_ref, z_ref, inv_ref, out_ref, va, vb, g = refs[-9:]
    side = scal[SIDE]
    depth, nx, ny = v_ref.shape

    @pl.when(scal[ROLE] == role)
    def _():
        row_last, lane_last = last_masks(nx, ny)
        zero = jnp.zeros((nx, ny), F32)
        for buf in (va, vb):
            buf[0] = zero
            buf[depth + ITERS + 1] = zero

        def fill(z, carry):
            at = ITERS * side + z
            va[1 + at] = v_ref[z]
            g[at] = (s_ref[z] + p_ref[z]) * inv_ref[at]
            return carry

        lax.fori_loop(0, depth, fill, 0, unroll=4)
        for q in range(ITERS):
            va[1 + jnp.where(side == 1, q, depth + q)] = vh_ref[q]
        for q in range(THIN):
            at = jnp.where(side == 1, 1 + q, depth + q)
            g[at] = (rim_ref[ITERS + q] + sum(ref[halo_at * side + q] for ref in ph_refs)) * inv_ref[at]
        src, dst = va, vb
        for k in range(ITERS):
            start = side * (1 + k)
            last = k == ITERS - 1

            def layer(j, carry, src=src, dst=dst, start=start, last=last):
                e = start + j
                new = g[e] + stencil(
                    src[e], src[e + 1], src[e + 2], c_ref[e], x_ref[e], y_ref[e], z_ref[e], row_last, lane_last
                )
                if last:
                    out_ref[j] = new
                else:
                    dst[e + 1] = new
                return carry

            count = depth + ITERS - 1 - k
            lax.fori_loop(0, count, layer, 0, unroll=True)
            src, dst = dst, src

    if pass_on:

        @pl.when(scal[ROLE] != role)
        def _():
            out_ref[...] = other_ref[...]

    for width, edge_ref in zip(widths, edge_refs):
        for q in range(width):
            edge_ref[q] = out_ref[jnp.where(side == 1, q, depth - width + q)]


def residual_kernel(scal, v_ref, h_ref, h2_ref, s_ref, c_ref, x_ref, y_ref, z_ref, diag_ref, p_ref, p2_ref, far_v, far_out, va, out_ref, sem):
    side = scal[SIDE]
    depth, nx, ny = v_ref.shape
    copies = [pltpu.make_async_copy(v_ref, far_v, sem.at[0])]
    copies[0].start()
    row_last, lane_last = last_masks(nx, ny)
    zero = jnp.zeros((nx, ny), F32)
    halo = h_ref[0] + h2_ref[0]
    va[0] = jnp.where(side == 1, halo, zero)
    va[depth + 1] = jnp.where(side == 1, zero, halo)
    for z in range(depth):
        va[1 + z] = v_ref[z]
    pieces = sem.shape[0] - 1
    size = depth // pieces
    for z in range(depth):
        e = ITERS * side + z
        here = va[1 + z]
        m = stencil(va[z], here, va[z + 2], c_ref[e], x_ref[e], y_ref[e], z_ref[e], row_last, lane_last)
        out_ref[z] = (s_ref[z] - diag_ref[z] * (here - m)) + (p_ref[z] + p2_ref[z])
        if (z + 1) % size == 0:
            part = pl.ds(z + 1 - size, size)
            copies.append(pltpu.make_async_copy(out_ref.at[part], far_out.at[part], sem.at[len(copies)]))
            copies[-1].start()
    for copy in copies:
        copy.wait()


def body(initial, source, diffusion, advection):
    tm, space = (lax.axis_size("tm"), lax.axis_size("space"))
    role = lax.axis_index("tm") % 2
    side = lax.axis_index("space")
    scalars = jnp.stack([role, side]).astype(jnp.int32)
    shape = initial.shape[1:]
    depth = shape[0]
    initial, source = (initial[0], source[0])

    def number(t, s):
        return (t % tm) * space + s

    def permute(value, pairs):
        return lax.ppermute(value, ("tm", "space"), pairs)

    sides = range(space)
    stride, group = ROW, ROW * RUNS
    even, odd = range(0, tm, 2), range(1, tm, 2)
    into_odd = [(number(t, s), number(t + 1, s)) for t in even for s in sides]
    into_even = [(number(t, s), number(t + 1, s)) for t in odd for s in sides]
    across_even = [(number(t, s), number(t, 1 - s)) for t in even for s in sides]
    across_odd = [(number(t, s), number(t, 1 - s)) for t in odd for s in sides]
    odd_across = [(number(t, s), number(t + 1, 1 - s)) for t in even for s in sides]
    even_across = [(number(t, s), number(t + 1, 1 - s)) for t in odd for s in sides]
    lower_odd = [(number(t, 1), number(t, 0)) for t in odd]
    lower_odd += [(number(t, 0), number(t - stride, 1)) for t in odd if t % group >= stride]
    for t in odd:
        if t % group >= group - stride:
            far_source = t - t % group + HELPER if t % stride < CORES else t - 1
            lower_odd.append((number(far_source, 0), number(t, 1)))
    back = [(number(t, s), number(t - 1, s)) for t in odd for s in sides]

    plane = shape[1:]
    ext = (depth + ITERS,) + plane
    padded = (depth + ITERS + 2,) + plane
    scratch = [pltpu.VMEM(padded, F32), pltpu.VMEM(padded, F32), pltpu.VMEM(ext, F32)]
    thin = (THIN,) + plane
    far = (initial, source, diffusion, advection)

    coef_edge, field_edge, thin_edge = call(
        pack_kernel, [(4 * THIN,) + plane, (ITERS + THIN,) + plane, thin], scalars, far=far, scratch=[pltpu.SemaphoreType.DMA((7,))]
    )
    si = permute(field_edge, across_even + across_odd)
    de = permute(thin_edge, even_across)
    b1 = permute(initial, into_even)
    sc = permute(coef_edge, lower_odd)
    a1 = permute(initial, into_odd)
    ao = permute(si, into_odd)

    def own(mine, *held):
        outs = [ext] * 5 + [shape] * 3
        room = [pltpu.VMEM(shape, F32), pltpu.VMEM((3,) + shape, F32), pltpu.SemaphoreType.DMA((4,))]
        aliases = {5 + i: i for i in range(len(held))}
        return call(functools.partial(own_kernel, mine, len(held)), outs, scalars, *held, far=far, scratch=room, aliases=aliases)

    held = own(1)
    ac = permute(sc, back)

    def rim(coefs, *sources):
        n = len(sources)
        return call(functools.partial(rim_kernel, n), [ext] * 5, scalars, *sources, *coefs, aliases={1 + n + i: i for i in range(5)})

    def sweep(mine, other, coefs, source_near, v, vh, p, *ph, widths=(), halo_at=0):
        outs = [shape] + [(w,) + plane for w in widths]
        extra = [other] if other is not None else []
        kernel = functools.partial(sweep_kernel, mine, other is not None, widths, halo_at)
        return call(kernel, outs, scalars, *extra, v, vh, source_near, si, p, *ph, *coefs, scratch=scratch)

    coefs = rim(held[:5], sc)
    x, xw, xt = sweep(1, None, coefs, held[7], held[6], si, a1, ao, widths=(ITERS, THIN), halo_at=1)
    b2 = permute(x, into_even)
    sx = permute(xw, across_odd)
    dx = permute(xt, even_across)
    *coefs, diag, initial_near, source_near = own(0, *coefs, *held[5:])
    coefs = rim(coefs, sc, ac)
    s1, yw, yt = sweep(0, x, coefs, source_near, initial_near, si, b1, de, widths=(ITERS, THIN))
    dy = permute(yt, odd_across)
    a2 = permute(s1, into_odd)
    z, zw = sweep(1, None, coefs, source_near, s1, sx, a2, dy, widths=(1,))
    b3 = permute(z, into_even)
    sy = permute(yw, across_even)
    sz = permute(zw, across_odd)
    s2, s2w = sweep(0, z, coefs, source_near, s1, sy, b2, dx, widths=(1,))
    a3 = permute(s2, into_odd)
    sw = permute(s2w, across_even)
    s2_far, residual = call(
        residual_kernel,
        [pltpu.HBM(shape, F32)] * 2,
        scalars,
        s2,
        sz,
        sw,
        source_near,
        *coefs[:4],
        diag,
        a3,
        b3,
        scratch=[pltpu.VMEM((depth + 2,) + plane, F32), pltpu.VMEM(shape, F32), pltpu.SemaphoreType.DMA((5,))],
    )
    return (s2_far[None], residual[None])


def solution(mesh):
    in_specs = (
        P("tm", "space", None, None),
        P("tm", "space", None, None),
        P("space", None, None),
        P(None, "space", None, None),
    )
    out_specs = (P("tm", "space", None, None), P("tm", "space", None, None))
    return jax.shard_map(body, mesh=mesh, in_specs=in_specs, out_specs=out_specs, check_vma=False)
```

```python
import functools

import jax
import jax.numpy as jnp
from jax import lax
from jax.experimental import pallas as pl
from jax.experimental.pallas import tpu as pltpu
from jax.sharding import PartitionSpec as P


ITERS = 4
THIN = ITERS - 1
HALO = ITERS + 1
F32 = jnp.float32
ROLE, SIDE = 0, 1
ROW, RUNS = 16, 4
HELPER = 6


def call(kernel, outs, scalars, *operands, far=(), scratch=(), aliases=None):
    far = [pltpu.with_memory_space_constraint(o, pltpu.HBM) for o in far]
    near = [pltpu.with_memory_space_constraint(o, pltpu.VMEM) for o in operands]
    return pl.pallas_call(
        kernel,
        out_shape=[o if not isinstance(o, tuple) else pltpu.VMEM(o, F32) for o in outs],
        in_specs=[pl.BlockSpec(memory_space=pltpu.SMEM)]
        + [pl.BlockSpec(memory_space=pltpu.HBM)] * len(far)
        + [pl.BlockSpec(memory_space=pltpu.VMEM)] * len(near),
        out_specs=[pl.BlockSpec(memory_space=pltpu.VMEM if isinstance(o, tuple) else pltpu.HBM) for o in outs],
        scratch_shapes=list(scratch),
        input_output_aliases=aliases or {},
        compiler_params=pltpu.CompilerParams(vmem_limit_bytes=16 * 1024 * 1024),
    )(scalars, *far, *near)


def pack_kernel(scal, init_ref, source_ref, spread_ref, upwind_ref, coef_out, field_out, thin_out, full_out, sem):
    side = scal[SIDE]
    depth = init_ref.shape[0]
    thin = pl.ds((1 - side) * (depth - THIN), THIN)
    wide = pl.ds((1 - side) * (depth - ITERS), ITERS)
    copies = [
        pltpu.make_async_copy(init_ref.at[wide], field_out.at[pl.ds(0, ITERS)], sem.at[0]),
        pltpu.make_async_copy(source_ref.at[wide], field_out.at[pl.ds(ITERS, ITERS)], sem.at[1]),
        pltpu.make_async_copy(init_ref.at[thin], thin_out, sem.at[6]),
        pltpu.make_async_copy(init_ref, full_out.at[pl.ds(0, depth)], sem.at[7]),
        pltpu.make_async_copy(spread_ref.at[wide], coef_out.at[pl.ds(0, ITERS)], sem.at[2]),
    ]
    for i in range(3):
        copies.append(pltpu.make_async_copy(upwind_ref.at[i, wide], coef_out.at[pl.ds((1 + i) * ITERS, ITERS)], sem.at[3 + i]))
    for copy in copies:
        copy.start()
    for copy in copies:
        copy.wait()


def weights(spread, ux, uy, uz, at, refs):
    c_ref, x_ref, y_ref, z_ref, inv_ref = refs
    nx, ny = spread.shape
    row = lax.broadcasted_iota(jnp.int32, (nx, ny), 0)
    lane = lax.broadcasted_iota(jnp.int32, (nx, ny), 1)
    diagonal = 1.0 + 6.0 * spread + (ux + uy + uz)
    inv = 1.0 / diagonal
    c_ref[at] = spread * inv
    x_ref[at] = jnp.where(row == 0, 0.0, (spread + ux) * inv)
    y_ref[at] = jnp.where(lane == 0, 0.0, (spread + uy) * inv)
    z_ref[at] = (spread + uz) * inv
    inv_ref[at] = inv
    return diagonal


def own_kernel(scal, source_far, spread_far, upwind_far, c_ref, x_ref, y_ref, z_ref, inv_ref, diag_ref, source_ref, spread_ref, upwind_ref, sem):
    side = scal[SIDE]
    depth = source_far.shape[0]
    copies = [
        pltpu.make_async_copy(spread_far, spread_ref, sem.at[0]),
        pltpu.make_async_copy(upwind_far, upwind_ref, sem.at[1]),
        pltpu.make_async_copy(source_far, source_ref, sem.at[2]),
    ]
    for copy in copies:
        copy.start()
    for copy in copies[:2]:
        copy.wait()

    def own(z, carry):
        diag_ref[z] = weights(
            spread_ref[z], upwind_ref[0, z], upwind_ref[1, z], upwind_ref[2, z], HALO * side + z, (c_ref, x_ref, y_ref, z_ref, inv_ref)
        )
        return carry

    lax.fori_loop(0, depth, own, 0, unroll=2)
    copies[2].wait()


def join_kernel(scal, field_ref, held_ref, full_ref):
    depth = full_ref.shape[0] - ITERS
    for q in range(ITERS):
        full_ref[depth + q] = field_ref[q]


def stencil(below, here, above, c, cx, cy, cz, row_last, lane_last):
    nx, ny = here.shape
    low_x = pltpu.roll(here, 1, 0)
    high_x = jnp.where(row_last, 0.0, pltpu.roll(here, nx - 1, 0))
    low_y = pltpu.roll(here, 1, 1)
    high_y = jnp.where(lane_last, 0.0, pltpu.roll(here, ny - 1, 1))
    return c * ((above + high_x) + high_y) + (cx * low_x + cz * below) + cy * low_y


def last_masks(nx, ny):
    row = lax.broadcasted_iota(jnp.int32, (nx, ny), 0)
    lane = lax.broadcasted_iota(jnp.int32, (nx, ny), 1)
    return row == nx - 1, lane == ny - 1


def sweep_kernel(role, pass_on, widths, extra, fields, v_at, p_halo, rims, scal, *refs):
    if pass_on:
        others, refs = refs[: 1 + extra], refs[1 + extra :]
    va, vb, g = refs[-3:]
    count = 4 + fields + 1 + rims + 5
    outs, rest = refs[count : count + 1 + extra], refs[count + 1 + extra : -3]
    edge_refs, made = rest[: len(widths)], rest[len(widths) :]
    v_ref, vh_ref, s_ref, rim_ref = refs[:4]
    p_refs, ph_ref = refs[4 : 4 + fields], refs[4 + fields]
    rim_sources = refs[5 + fields : 5 + fields + rims]
    c_ref, x_ref, y_ref, z_ref, inv_ref = made if rims else refs[count - 5 : count]
    p_at, reach = p_halo
    out_ref = outs[0]
    side = scal[SIDE]
    depth, nx, ny = out_ref.shape
    held_v, held_f = ITERS + extra, THIN + extra

    @pl.when(scal[ROLE] == role)
    def _():
        for q in range(ITERS if rims else 0):
            at = jnp.where(side == 1, HALO - ITERS + q, depth + q)
            parts = [sum(ref[i * ITERS + q] for ref in rim_sources) for i in range(4)]
            weights(*parts, at, (c_ref, x_ref, y_ref, z_ref, inv_ref))
        row_last, lane_last = last_masks(nx, ny)
        zero = jnp.zeros((nx, ny), F32)
        for buf in (va, vb):
            buf[0] = zero
            buf[depth + HALO + 1] = zero

        def fill(z, carry):
            at = HALO * side + z
            va[1 + at] = v_ref[z]
            g[at] = (s_ref[z] + sum(ref[z] for ref in p_refs)) * inv_ref[at]
            return carry

        lax.fori_loop(0, depth, fill, 0, unroll=4)
        for q in range(held_v):
            va[1 + jnp.where(side == 1, HALO - held_v + q, depth + q)] = vh_ref[v_at + q]
        for q in range(held_f):
            at = jnp.where(side == 1, HALO - held_f + q, depth + q)
            rim = rim_ref[ITERS + (ITERS - held_f) * side + q]
            g[at] = (rim + ph_ref[p_at + (reach - held_f) * side + q]) * inv_ref[at]
        src, dst = va, vb
        for k in range(ITERS):
            start = side * (HALO - held_f + k)
            direct = k == ITERS - 1 and extra == 0

            def layer(j, carry, src=src, dst=dst, start=start, direct=direct):
                e = start + j
                new = g[e] + stencil(
                    src[e], src[e + 1], src[e + 2], c_ref[e], x_ref[e], y_ref[e], z_ref[e], row_last, lane_last
                )
                if direct:
                    out_ref[j] = new
                else:
                    dst[e + 1] = new
                return carry

            lax.fori_loop(0, depth + held_f - k, layer, 0, unroll=True)
            src, dst = dst, src
        if extra:
            for z in range(depth):
                out_ref[z] = src[1 + HALO * side + z]
            outs[1][0] = src[1 + jnp.where(side == 1, HALO - 1, depth)]

    if pass_on:

        @pl.when(scal[ROLE] != role)
        def _():
            for other, out in zip(others, outs):
                out[...] = other[...]

    for width, edge_ref in zip(widths, edge_refs):
        for q in range(width):
            edge_ref[q] = out_ref[jnp.where(side == 1, q, depth - width + q)]


def residual_kernel(scal, v_ref, h_ref, s_ref, c_ref, x_ref, y_ref, z_ref, diag_ref, p_ref, p2_ref, far_v, far_out, va, out_ref, sem):
    side = scal[SIDE]
    depth, nx, ny = v_ref.shape
    copies = [pltpu.make_async_copy(v_ref, far_v, sem.at[0])]
    copies[0].start()
    row_last, lane_last = last_masks(nx, ny)
    zero = jnp.zeros((nx, ny), F32)
    halo = h_ref[0]
    va[0] = jnp.where(side == 1, halo, zero)
    va[depth + 1] = jnp.where(side == 1, zero, halo)
    for z in range(depth):
        va[1 + z] = v_ref[z]
    pieces = sem.shape[0] - 1
    size = depth // pieces
    for z in range(depth):
        e = HALO * side + z
        here = va[1 + z]
        m = stencil(va[z], here, va[z + 2], c_ref[e], x_ref[e], y_ref[e], z_ref[e], row_last, lane_last)
        out_ref[z] = (s_ref[z] - diag_ref[z] * (here - m)) + (p_ref[z] + p2_ref[z])
        if (z + 1) % size == 0:
            part = pl.ds(z + 1 - size, size)
            copies.append(pltpu.make_async_copy(out_ref.at[part], far_out.at[part], sem.at[len(copies)]))
            copies[-1].start()
    for copy in copies:
        copy.wait()


def body(initial, source, diffusion, advection):
    tm, space = (lax.axis_size("tm"), lax.axis_size("space"))
    role = lax.axis_index("tm") % 2
    side = lax.axis_index("space")
    scalars = jnp.stack([role, side]).astype(jnp.int32)
    shape = initial.shape[1:]
    depth = shape[0]
    initial, source = (initial[0], source[0])

    def number(t, s):
        return (t % tm) * space + s

    def permute(value, pairs):
        return lax.ppermute(value, ("tm", "space"), pairs)

    sides = range(space)
    stride, group = ROW, ROW * RUNS
    even, odd = range(0, tm, 2), range(1, tm, 2)
    into_odd = [(number(t, s), number(t + 1, s)) for t in even for s in sides]
    into_even = [(number(t, s), number(t + 1, s)) for t in odd for s in sides]
    short_even = [(number(t, s), number(t + 1, s)) for t in odd for s in sides if t % ROW < ROW - 1 or s == 0]
    last = [t for t in odd if t % ROW == ROW - 1]
    last_along = [(number(t, 1), number(t + ROW, 1)) for t in last]
    last_around = [(number(t, 1), number(t + 1 - ROW, 1)) for t in last]
    across_even = [(number(t, s), number(t, 1 - s)) for t in even for s in sides]
    across_odd = [(number(t, s), number(t, 1 - s)) for t in odd for s in sides]
    odd_across = [(number(t, s), number(t + 1, 1 - s)) for t in even for s in sides]
    even_across = [(number(t, s), number(t + 1, 1 - s)) for t in odd for s in sides]
    lower_odd = []
    for t in odd:
        run, first = (t % group) // stride, t % stride == 1
        lower_odd.append((number(t, 1) if first else number(t - stride, 1) if run else number(t - 1, 1), number(t, 0)))
        if run < RUNS - 1:
            lower_odd.append((number(t + stride, 0), number(t, 1)))
        else:
            lower_odd.append((number(t - t % group + HELPER if first else t - 1, 0), number(t, 1)))
    back = [(number(t, s), number(t - 1, s)) for t in odd for s in sides]

    plane = shape[1:]
    ext = (depth + HALO,) + plane
    padded = (depth + HALO + 2,) + plane
    scratch = [pltpu.VMEM(padded, F32), pltpu.VMEM(padded, F32), pltpu.VMEM(ext, F32)]
    thin = (THIN,) + plane
    far = (initial, source, diffusion, advection)

    coef_edge, field_edge, thin_edge, full = call(
        pack_kernel,
        [(4 * ITERS,) + plane, (2 * ITERS,) + plane, thin, (depth + ITERS,) + plane],
        scalars,
        far=far,
        scratch=[pltpu.SemaphoreType.DMA((8,))],
    )
    si = permute(field_edge, across_even + across_odd)
    de = permute(thin_edge, even_across)
    b1 = permute(initial, into_even)
    sc = permute(coef_edge, lower_odd)
    *coefs, diag, source_near = call(
        own_kernel,
        [ext] * 5 + [shape] * 2,
        scalars,
        far=far[1:],
        scratch=[pltpu.VMEM(shape, F32), pltpu.VMEM((3,) + shape, F32), pltpu.SemaphoreType.DMA((3,))],
    )
    (full,) = call(join_kernel, [(depth + ITERS,) + plane], scalars, si, full, aliases={2: 0})
    a1 = permute(full, into_odd)
    ac = permute(sc, back)

    def sweep(mine, others, v, vh, p, ph, p_halo, v_at=0, widths=(), extra=0, rims=()):
        nonlocal coefs
        outs = [shape] + [(w,) + plane for w in (1,) * extra + widths]
        kernel = functools.partial(sweep_kernel, mine, bool(others), widths, extra, len(p), v_at, p_halo, len(rims))
        operands = (*others, v, vh, source_near, si, *p, ph, *rims)
        made = [ext] * 5 if rims else []
        aliases = {1 + len(operands) + i: len(outs) + i for i in range(len(made))}
        out = call(kernel, outs + made, scalars, *operands, *coefs, scratch=scratch, aliases=aliases)
        if rims:
            out, coefs = out[:-5], out[-5:]
        return out

    x, xw, xt = sweep(1, (), full, full, (a1,), a1, (depth, ITERS), depth, (HALO, ITERS), rims=(sc,))
    b2 = permute(x, short_even)
    sx = permute(xw, across_odd)
    zh = permute(x, last_along)
    s1, yw = sweep(0, (x,), full, full, (b1,), de, (0, THIN), depth, (HALO,), rims=(ac,))
    dy = permute(yw, odd_across)
    a2 = permute(s1, into_odd)
    dx = permute(xt, even_across)
    yh = permute(zh, last_around)
    z, zh1 = sweep(1, (), s1, sx, (a2,), dy, (0, HALO), extra=1)
    b3 = permute(z, into_even)
    ey = permute(dy, back)
    s2, s2h = sweep(0, (z, zh1), s1, ey, (b2, yh), dx, (0, ITERS), extra=1)
    a3 = permute(s2, into_odd)
    s2_far, residual = call(
        residual_kernel,
        [pltpu.HBM(shape, F32)] * 2,
        scalars,
        s2,
        s2h,
        source_near,
        *coefs[:4],
        diag,
        a3,
        b3,
        scratch=[pltpu.VMEM((depth + 2,) + plane, F32), pltpu.VMEM(shape, F32), pltpu.SemaphoreType.DMA((5,))],
    )
    return (s2_far[None], residual[None])


def solution(mesh):
    in_specs = (
        P("tm", "space", None, None),
        P("tm", "space", None, None),
        P("space", None, None),
        P(None, "space", None, None),
    )
    out_specs = (P("tm", "space", None, None), P("tm", "space", None, None))
    return jax.shard_map(body, mesh=mesh, in_specs=in_specs, out_specs=out_specs, check_vma=False)
```

```python
import functools

import jax
import jax.numpy as jnp
from jax import lax
from jax.experimental import pallas as pl
from jax.experimental.pallas import tpu as pltpu
from jax.sharding import PartitionSpec as P


ITERS = 4
THIN = ITERS - 1
HALO = ITERS + 1
F32 = jnp.float32
ROLE, SIDE = 0, 1
ROW, RUNS, CORES = 16, 4, 2
HELPER = 6


def call(kernel, outs, scalars, *operands, far=(), scratch=(), aliases=None):
    far = [pltpu.with_memory_space_constraint(o, pltpu.HBM) for o in far]
    near = [pltpu.with_memory_space_constraint(o, pltpu.VMEM) for o in operands]
    return pl.pallas_call(
        kernel,
        out_shape=[o if not isinstance(o, tuple) else pltpu.VMEM(o, F32) for o in outs],
        in_specs=[pl.BlockSpec(memory_space=pltpu.SMEM)]
        + [pl.BlockSpec(memory_space=pltpu.HBM)] * len(far)
        + [pl.BlockSpec(memory_space=pltpu.VMEM)] * len(near),
        out_specs=[pl.BlockSpec(memory_space=pltpu.VMEM if isinstance(o, tuple) else pltpu.HBM) for o in outs],
        scratch_shapes=list(scratch),
        input_output_aliases=aliases or {},
        compiler_params=pltpu.CompilerParams(vmem_limit_bytes=16 * 1024 * 1024),
    )(scalars, *far, *near)


def pack_kernel(scal, init_ref, source_ref, spread_ref, upwind_ref, coef_out, field_out, thin_out, sem):
    side = scal[SIDE]
    depth = init_ref.shape[0]
    thin = pl.ds((1 - side) * (depth - THIN), THIN)
    wide = pl.ds((1 - side) * (depth - ITERS), ITERS)
    copies = [
        pltpu.make_async_copy(init_ref.at[wide], field_out.at[pl.ds(0, ITERS)], sem.at[0]),
        pltpu.make_async_copy(source_ref.at[wide], field_out.at[pl.ds(ITERS, ITERS)], sem.at[1]),
        pltpu.make_async_copy(init_ref.at[thin], thin_out, sem.at[6]),
        pltpu.make_async_copy(spread_ref.at[wide], coef_out.at[pl.ds(0, ITERS)], sem.at[2]),
    ]
    for i in range(3):
        copies.append(pltpu.make_async_copy(upwind_ref.at[i, wide], coef_out.at[pl.ds((1 + i) * ITERS, ITERS)], sem.at[3 + i]))
    for copy in copies:
        copy.start()
    for copy in copies:
        copy.wait()


def weights(spread, ux, uy, uz, at, refs):
    c_ref, x_ref, y_ref, z_ref, inv_ref = refs
    nx, ny = spread.shape
    row = lax.broadcasted_iota(jnp.int32, (nx, ny), 0)
    lane = lax.broadcasted_iota(jnp.int32, (nx, ny), 1)
    diagonal = 1.0 + 6.0 * spread + (ux + uy + uz)
    inv = 1.0 / diagonal
    c_ref[at] = spread * inv
    x_ref[at] = jnp.where(row == 0, 0.0, (spread + ux) * inv)
    y_ref[at] = jnp.where(lane == 0, 0.0, (spread + uy) * inv)
    z_ref[at] = (spread + uz) * inv
    inv_ref[at] = inv
    return diagonal


def own_kernel(scal, init_far, source_far, spread_far, upwind_far, c_ref, x_ref, y_ref, z_ref, inv_ref, diag_ref, source_ref, full_ref, spread_ref, upwind_ref, sem):
    side = scal[SIDE]
    depth = source_far.shape[0]
    copies = [
        pltpu.make_async_copy(spread_far, spread_ref, sem.at[0]),
        pltpu.make_async_copy(upwind_far, upwind_ref, sem.at[1]),
        pltpu.make_async_copy(source_far, source_ref, sem.at[2]),
        pltpu.make_async_copy(init_far, full_ref.at[pl.ds(0, depth)], sem.at[3]),
    ]
    for copy in copies:
        copy.start()
    for copy in copies[:2]:
        copy.wait()

    def own(z, carry):
        diag_ref[z] = weights(
            spread_ref[z], upwind_ref[0, z], upwind_ref[1, z], upwind_ref[2, z], HALO * side + z, (c_ref, x_ref, y_ref, z_ref, inv_ref)
        )
        return carry

    lax.fori_loop(0, depth, own, 0, unroll=2)
    for copy in copies[2:]:
        copy.wait()


def join_kernel(scal, field_ref, held_ref, full_ref):
    depth = full_ref.shape[0] - ITERS
    for q in range(ITERS):
        full_ref[depth + q] = field_ref[q]


def stencil(below, here, above, c, cx, cy, cz, row_last, lane_last):
    nx, ny = here.shape
    low_x = pltpu.roll(here, 1, 0)
    high_x = jnp.where(row_last, 0.0, pltpu.roll(here, nx - 1, 0))
    low_y = pltpu.roll(here, 1, 1)
    high_y = jnp.where(lane_last, 0.0, pltpu.roll(here, ny - 1, 1))
    return c * ((above + high_x) + high_y) + (cx * low_x + cz * below) + cy * low_y


def last_masks(nx, ny):
    row = lax.broadcasted_iota(jnp.int32, (nx, ny), 0)
    lane = lax.broadcasted_iota(jnp.int32, (nx, ny), 1)
    return row == nx - 1, lane == ny - 1


def sweep_kernel(role, pass_on, widths, extra, fields, v_at, p_halo, rims, scal, *refs):
    if pass_on:
        others, refs = refs[: 1 + extra], refs[1 + extra :]
    va, vb, g = refs[-3:]
    count = 4 + fields + 1 + rims + 5
    outs, rest = refs[count : count + 1 + extra], refs[count + 1 + extra : -3]
    edge_refs, made = rest[: len(widths)], rest[len(widths) :]
    v_ref, vh_ref, s_ref, rim_ref = refs[:4]
    p_refs, ph_ref = refs[4 : 4 + fields], refs[4 + fields]
    rim_sources = refs[5 + fields : 5 + fields + rims]
    c_ref, x_ref, y_ref, z_ref, inv_ref = made if rims else refs[count - 5 : count]
    p_at, reach = p_halo
    out_ref = outs[0]
    side = scal[SIDE]
    depth, nx, ny = out_ref.shape
    held_v, held_f = ITERS + extra, THIN + extra

    @pl.when(scal[ROLE] == role)
    def _():
        for q in range(ITERS if rims else 0):
            at = jnp.where(side == 1, HALO - ITERS + q, depth + q)
            parts = [sum(ref[i * ITERS + q] for ref in rim_sources) for i in range(4)]
            weights(*parts, at, (c_ref, x_ref, y_ref, z_ref, inv_ref))
        row_last, lane_last = last_masks(nx, ny)
        zero = jnp.zeros((nx, ny), F32)
        for buf in (va, vb):
            buf[0] = zero
            buf[depth + HALO + 1] = zero

        def fill(z, carry):
            at = HALO * side + z
            va[1 + at] = v_ref[z]
            g[at] = (s_ref[z] + sum(ref[z] for ref in p_refs)) * inv_ref[at]
            return carry

        lax.fori_loop(0, depth, fill, 0, unroll=4)
        for q in range(held_v):
            va[1 + jnp.where(side == 1, HALO - held_v + q, depth + q)] = vh_ref[v_at + q]
        for q in range(held_f):
            at = jnp.where(side == 1, HALO - held_f + q, depth + q)
            rim = rim_ref[ITERS + (ITERS - held_f) * side + q]
            g[at] = (rim + ph_ref[p_at + (reach - held_f) * side + q]) * inv_ref[at]
        src, dst = va, vb
        for k in range(ITERS):
            start = side * (HALO - held_f + k)
            direct = k == ITERS - 1 and extra == 0

            def layer(j, carry, src=src, dst=dst, start=start, direct=direct):
                e = start + j
                new = g[e] + stencil(
                    src[e], src[e + 1], src[e + 2], c_ref[e], x_ref[e], y_ref[e], z_ref[e], row_last, lane_last
                )
                if direct:
                    out_ref[j] = new
                else:
                    dst[e + 1] = new
                return carry

            lax.fori_loop(0, depth + held_f - k, layer, 0, unroll=True)
            src, dst = dst, src
        if extra:
            for z in range(depth):
                out_ref[z] = src[1 + HALO * side + z]
            outs[1][0] = src[1 + jnp.where(side == 1, HALO - 1, depth)]

    if pass_on:

        @pl.when(scal[ROLE] != role)
        def _():
            for other, out in zip(others, outs):
                out[...] = other[...]

    for width, edge_ref in zip(widths, edge_refs):
        for q in range(width):
            edge_ref[q] = out_ref[jnp.where(side == 1, q, depth - width + q)]


def residual_kernel(scal, v_ref, h_ref, s_ref, c_ref, x_ref, y_ref, z_ref, diag_ref, p_ref, p2_ref, far_v, far_out, va, out_ref, sem):
    side = scal[SIDE]
    depth, nx, ny = v_ref.shape
    copies = [pltpu.make_async_copy(v_ref, far_v, sem.at[0])]
    copies[0].start()
    row_last, lane_last = last_masks(nx, ny)
    zero = jnp.zeros((nx, ny), F32)
    halo = h_ref[0]
    va[0] = jnp.where(side == 1, halo, zero)
    va[depth + 1] = jnp.where(side == 1, zero, halo)
    for z in range(depth):
        va[1 + z] = v_ref[z]
    pieces = sem.shape[0] - 1
    size = depth // pieces
    for z in range(depth):
        e = HALO * side + z
        here = va[1 + z]
        m = stencil(va[z], here, va[z + 2], c_ref[e], x_ref[e], y_ref[e], z_ref[e], row_last, lane_last)
        out_ref[z] = (s_ref[z] - diag_ref[z] * (here - m)) + (p_ref[z] + p2_ref[z])
        if (z + 1) % size == 0:
            part = pl.ds(z + 1 - size, size)
            copies.append(pltpu.make_async_copy(out_ref.at[part], far_out.at[part], sem.at[len(copies)]))
            copies[-1].start()
    for copy in copies:
        copy.wait()


def body(initial, source, diffusion, advection):
    tm, space = (lax.axis_size("tm"), lax.axis_size("space"))
    role = lax.axis_index("tm") % 2
    side = lax.axis_index("space")
    scalars = jnp.stack([role, side]).astype(jnp.int32)
    shape = initial.shape[1:]
    depth = shape[0]
    initial, source = (initial[0], source[0])

    def number(t, s):
        return (t % tm) * space + s

    def permute(value, pairs):
        return lax.ppermute(value, ("tm", "space"), pairs)

    sides = range(space)
    stride, group = ROW, ROW * RUNS
    even, odd = range(0, tm, 2), range(1, tm, 2)
    into_odd = [(number(t, s), number(t + 1, s)) for t in even for s in sides]
    into_even = [(number(t, s), number(t + 1, s)) for t in odd for s in sides]
    short_even = [(number(t, s), number(t + 1, s)) for t in odd for s in sides if t % ROW < ROW - 1 or s == 0]
    last = [t for t in odd if t % ROW == ROW - 1]
    last_along = [(number(t, 1), number(t + 1 + CORES, 1)) for t in last]
    last_around = [(number(t + 1 + CORES, 1), number(t + 1, 1)) for t in last]
    across_even = [(number(t, s), number(t, 1 - s)) for t in even for s in sides]
    across_odd = [(number(t, s), number(t, 1 - s)) for t in odd for s in sides]
    odd_across = [(number(t, s), number(t + 1, 1 - s)) for t in even for s in sides]
    even_across = [(number(t, s), number(t + 1, 1 - s)) for t in odd for s in sides]
    lower_odd = []
    for t in odd:
        run, first = (t % group) // stride, t % stride == 1
        lower_odd.append((number(t, 1) if first else number(t - stride, 1) if run else number(t - 1, 1), number(t, 0)))
        if run < RUNS - 1:
            lower_odd.append((number(t + stride, 0), number(t, 1)))
        else:
            end = t % stride == stride - 1
            base = t - t % group
            lower_odd.append((number(base + HELPER if first else base + stride - CORES if end else t - 1, 0), number(t, 1)))
    back = [(number(t, s), number(t - 1, s)) for t in odd for s in sides]

    plane = shape[1:]
    ext = (depth + HALO,) + plane
    padded = (depth + HALO + 2,) + plane
    scratch = [pltpu.VMEM(padded, F32), pltpu.VMEM(padded, F32), pltpu.VMEM(ext, F32)]
    thin = (THIN,) + plane
    far = (initial, source, diffusion, advection)

    coef_edge, field_edge, thin_edge = call(
        pack_kernel, [(4 * ITERS,) + plane, (2 * ITERS,) + plane, thin], scalars, far=far, scratch=[pltpu.SemaphoreType.DMA((7,))]
    )
    si = permute(field_edge, across_even + across_odd)
    de = permute(thin_edge, even_across)
    b1 = permute(initial, into_even)
    sc = permute(coef_edge, lower_odd)
    *coefs, diag, source_near, full = call(
        own_kernel,
        [ext] * 5 + [shape] * 2 + [(depth + ITERS,) + plane],
        scalars,
        far=far,
        scratch=[pltpu.VMEM(shape, F32), pltpu.VMEM((3,) + shape, F32), pltpu.SemaphoreType.DMA((4,))],
    )
    (full,) = call(join_kernel, [(depth + ITERS,) + plane], scalars, si, full, aliases={2: 0})
    a1 = permute(full, into_odd)
    ac = permute(sc, back)

    def sweep(mine, others, v, vh, p, ph, p_halo, v_at=0, widths=(), extra=0, rims=()):
        nonlocal coefs
        outs = [shape] + [(w,) + plane for w in (1,) * extra + widths]
        kernel = functools.partial(sweep_kernel, mine, bool(others), widths, extra, len(p), v_at, p_halo, len(rims))
        operands = (*others, v, vh, source_near, si, *p, ph, *rims)
        made = [ext] * 5 if rims else []
        aliases = {1 + len(operands) + i: len(outs) + i for i in range(len(made))}
        out = call(kernel, outs + made, scalars, *operands, *coefs, scratch=scratch, aliases=aliases)
        if rims:
            out, coefs = out[:-5], out[-5:]
        return out

    x, xw, xt = sweep(1, (), full, full, (a1,), a1, (depth, ITERS), depth, (HALO, ITERS), rims=(sc,))
    b2 = permute(x, short_even)
    sx = permute(xw, across_odd)
    zh = permute(x, last_along)
    s1, yw = sweep(0, (x,), full, full, (b1,), de, (0, THIN), depth, (HALO,), rims=(ac,))
    dy = permute(yw, odd_across)
    a2 = permute(s1, into_odd)
    dx = permute(xt, even_across)
    yh = permute(zh, last_around)
    z, zh1 = sweep(1, (), s1, sx, (a2,), dy, (0, HALO), extra=1)
    b3 = permute(z, into_even)
    ey = permute(dy, back)
    s2, s2h = sweep(0, (z, zh1), s1, ey, (b2, yh), dx, (0, ITERS), extra=1)
    a3 = permute(s2, into_odd)
    s2_far, residual = call(
        residual_kernel,
        [pltpu.HBM(shape, F32)] * 2,
        scalars,
        s2,
        s2h,
        source_near,
        *coefs[:4],
        diag,
        a3,
        b3,
        scratch=[pltpu.VMEM((depth + 2,) + plane, F32), pltpu.VMEM(shape, F32), pltpu.SemaphoreType.DMA((5,))],
    )
    return (s2_far[None], residual[None])


def solution(mesh):
    in_specs = (
        P("tm", "space", None, None),
        P("tm", "space", None, None),
        P("space", None, None),
        P(None, "space", None, None),
    )
    out_specs = (P("tm", "space", None, None), P("tm", "space", None, None))
    return jax.shard_map(body, mesh=mesh, in_specs=in_specs, out_specs=out_specs, check_vma=False)
```

```python
import functools

import jax
import jax.numpy as jnp
from jax import lax
from jax.experimental import pallas as pl
from jax.experimental.pallas import tpu as pltpu
from jax.sharding import PartitionSpec as P


ITERS = 4
THIN = ITERS - 1
HALO = ITERS + 1
F32 = jnp.float32
ROLE, SIDE = 0, 1
ROW, RUNS, CORES = 16, 4, 2
HELPER = 6


def call(kernel, outs, scalars, *operands, far=(), scratch=(), aliases=None):
    far = [pltpu.with_memory_space_constraint(o, pltpu.HBM) for o in far]
    near = [pltpu.with_memory_space_constraint(o, pltpu.VMEM) for o in operands]
    return pl.pallas_call(
        kernel,
        out_shape=[o if not isinstance(o, tuple) else pltpu.VMEM(o, F32) for o in outs],
        in_specs=[pl.BlockSpec(memory_space=pltpu.SMEM)]
        + [pl.BlockSpec(memory_space=pltpu.HBM)] * len(far)
        + [pl.BlockSpec(memory_space=pltpu.VMEM)] * len(near),
        out_specs=[pl.BlockSpec(memory_space=pltpu.VMEM if isinstance(o, tuple) else pltpu.HBM) for o in outs],
        scratch_shapes=list(scratch),
        input_output_aliases=aliases or {},
        compiler_params=pltpu.CompilerParams(vmem_limit_bytes=16 * 1024 * 1024),
    )(scalars, *far, *near)


def pack_kernel(scal, init_ref, source_ref, spread_ref, upwind_ref, coef_out, field_out, thin_out, sem):
    side = scal[SIDE]
    depth = init_ref.shape[0]
    thin = pl.ds((1 - side) * (depth - THIN), THIN)
    wide = pl.ds((1 - side) * (depth - ITERS), ITERS)
    copies = [
        pltpu.make_async_copy(init_ref.at[wide], field_out.at[pl.ds(0, ITERS)], sem.at[0]),
        pltpu.make_async_copy(source_ref.at[wide], field_out.at[pl.ds(ITERS, ITERS)], sem.at[1]),
        pltpu.make_async_copy(init_ref.at[thin], thin_out, sem.at[6]),
        pltpu.make_async_copy(spread_ref.at[wide], coef_out.at[pl.ds(0, ITERS)], sem.at[2]),
    ]
    for i in range(3):
        copies.append(pltpu.make_async_copy(upwind_ref.at[i, wide], coef_out.at[pl.ds((1 + i) * ITERS, ITERS)], sem.at[3 + i]))
    for copy in copies:
        copy.start()
    for copy in copies:
        copy.wait()


def weights(spread, ux, uy, uz, at, refs):
    c_ref, x_ref, y_ref, z_ref, inv_ref = refs
    nx, ny = spread.shape
    row = lax.broadcasted_iota(jnp.int32, (nx, ny), 0)
    lane = lax.broadcasted_iota(jnp.int32, (nx, ny), 1)
    diagonal = 1.0 + 6.0 * spread + (ux + uy + uz)
    inv = 1.0 / diagonal
    c_ref[at] = spread * inv
    x_ref[at] = jnp.where(row == 0, 0.0, (spread + ux) * inv)
    y_ref[at] = jnp.where(lane == 0, 0.0, (spread + uy) * inv)
    z_ref[at] = (spread + uz) * inv
    inv_ref[at] = inv
    return diagonal


def own_kernel(scal, init_far, source_far, spread_far, upwind_far, c_ref, x_ref, y_ref, z_ref, inv_ref, diag_ref, source_ref, full_ref, spread_ref, upwind_ref, sem):
    side = scal[SIDE]
    depth = source_far.shape[0]
    copies = [
        pltpu.make_async_copy(spread_far, spread_ref, sem.at[0]),
        pltpu.make_async_copy(upwind_far, upwind_ref, sem.at[1]),
        pltpu.make_async_copy(source_far, source_ref, sem.at[2]),
        pltpu.make_async_copy(init_far, full_ref.at[pl.ds(0, depth)], sem.at[3]),
    ]
    for copy in copies:
        copy.start()
    for copy in copies[:2]:
        copy.wait()

    def own(z, carry):
        diag_ref[z] = weights(
            spread_ref[z], upwind_ref[0, z], upwind_ref[1, z], upwind_ref[2, z], HALO * side + z, (c_ref, x_ref, y_ref, z_ref, inv_ref)
        )
        return carry

    lax.fori_loop(0, depth, own, 0, unroll=2)
    for copy in copies[2:]:
        copy.wait()


def join_kernel(scal, field_ref, held_ref, full_ref):
    depth = full_ref.shape[0] - ITERS
    for q in range(ITERS):
        full_ref[depth + q] = field_ref[q]


def stencil(below, here, above, c, cx, cy, cz, row_last, lane_last):
    nx, ny = here.shape
    low_x = pltpu.roll(here, 1, 0)
    high_x = jnp.where(row_last, 0.0, pltpu.roll(here, nx - 1, 0))
    low_y = pltpu.roll(here, 1, 1)
    high_y = jnp.where(lane_last, 0.0, pltpu.roll(here, ny - 1, 1))
    return c * ((above + high_x) + high_y) + (cx * low_x + cz * below) + cy * low_y


def last_masks(nx, ny):
    row = lax.broadcasted_iota(jnp.int32, (nx, ny), 0)
    lane = lax.broadcasted_iota(jnp.int32, (nx, ny), 1)
    return row == nx - 1, lane == ny - 1


def sweep_kernel(role, pass_on, widths, extra, fields, v_at, p_halo, rims, scal, *refs):
    if pass_on:
        others, refs = refs[: 1 + extra], refs[1 + extra :]
    va, vb, g = refs[-3:]
    count = 4 + fields + 1 + rims + 5
    outs, rest = refs[count : count + 1 + extra], refs[count + 1 + extra : -3]
    edge_refs, made = rest[: len(widths)], rest[len(widths) :]
    v_ref, vh_ref, s_ref, rim_ref = refs[:4]
    p_refs, ph_ref = refs[4 : 4 + fields], refs[4 + fields]
    rim_sources = refs[5 + fields : 5 + fields + rims]
    c_ref, x_ref, y_ref, z_ref, inv_ref = made if rims else refs[count - 5 : count]
    p_at, reach = p_halo
    out_ref = outs[0]
    side = scal[SIDE]
    depth, nx, ny = out_ref.shape
    held_v, held_f = ITERS + extra, THIN + extra

    @pl.when(scal[ROLE] == role)
    def _():
        for q in range(ITERS if rims else 0):
            at = jnp.where(side == 1, HALO - ITERS + q, depth + q)
            parts = [sum(ref[i * ITERS + q] for ref in rim_sources) for i in range(4)]
            weights(*parts, at, (c_ref, x_ref, y_ref, z_ref, inv_ref))
        row_last, lane_last = last_masks(nx, ny)
        zero = jnp.zeros((nx, ny), F32)
        for buf in (va, vb):
            buf[0] = zero
            buf[depth + HALO + 1] = zero

        def fill(z, carry):
            at = HALO * side + z
            va[1 + at] = v_ref[z]
            g[at] = (s_ref[z] + sum(ref[z] for ref in p_refs)) * inv_ref[at]
            return carry

        lax.fori_loop(0, depth, fill, 0, unroll=4)
        for q in range(held_v):
            va[1 + jnp.where(side == 1, HALO - held_v + q, depth + q)] = vh_ref[v_at + q]
        for q in range(held_f):
            at = jnp.where(side == 1, HALO - held_f + q, depth + q)
            rim = rim_ref[ITERS + (ITERS - held_f) * side + q]
            g[at] = (rim + ph_ref[p_at + (reach - held_f) * side + q]) * inv_ref[at]
        src, dst = va, vb
        for k in range(ITERS):
            start = side * (HALO - held_f + k)
            direct = k == ITERS - 1 and extra == 0

            def layer(j, carry, src=src, dst=dst, start=start, direct=direct):
                e = start + j
                new = g[e] + stencil(
                    src[e], src[e + 1], src[e + 2], c_ref[e], x_ref[e], y_ref[e], z_ref[e], row_last, lane_last
                )
                if direct:
                    out_ref[j] = new
                else:
                    dst[e + 1] = new
                return carry

            lax.fori_loop(0, depth + held_f - k, layer, 0, unroll=True)
            src, dst = dst, src
        if extra:
            for z in range(depth):
                out_ref[z] = src[1 + HALO * side + z]
            outs[1][0] = src[1 + jnp.where(side == 1, HALO - 1, depth)]

    if pass_on:

        @pl.when(scal[ROLE] != role)
        def _():
            for other, out in zip(others, outs):
                out[...] = other[...]

    for width, edge_ref in zip(widths, edge_refs):
        for q in range(width):
            edge_ref[q] = out_ref[jnp.where(side == 1, q, depth - width + q)]


def defect_kernel(scal, v_ref, h_ref, s_ref, c_ref, x_ref, y_ref, z_ref, diag_ref, far_v, out_ref, va, sem):
    side = scal[SIDE]
    depth, nx, ny = v_ref.shape
    copy = pltpu.make_async_copy(v_ref, far_v, sem)
    copy.start()
    row_last, lane_last = last_masks(nx, ny)
    zero = jnp.zeros((nx, ny), F32)
    halo = h_ref[0]
    va[0] = jnp.where(side == 1, halo, zero)
    va[depth + 1] = jnp.where(side == 1, zero, halo)
    for z in range(depth):
        va[1 + z] = v_ref[z]
    for z in range(depth):
        e = HALO * side + z
        here = va[1 + z]
        m = stencil(va[z], here, va[z + 2], c_ref[e], x_ref[e], y_ref[e], z_ref[e], row_last, lane_last)
        out_ref[z] = s_ref[z] - diag_ref[z] * (here - m)
    copy.wait()


def add_kernel(scal, d_ref, p_ref, p2_ref, far_out, out_ref, sem):
    pieces = sem.shape[0]
    size = out_ref.shape[0] // pieces
    copies = []
    for i in range(pieces):
        part = pl.ds(i * size, size)
        for z in range(i * size, (i + 1) * size):
            out_ref[z] = d_ref[z] + (p_ref[z] + p2_ref[z])
        copies.append(pltpu.make_async_copy(out_ref.at[part], far_out.at[part], sem.at[i]))
        copies[-1].start()
    for copy in copies:
        copy.wait()


def body(initial, source, diffusion, advection):
    tm, space = (lax.axis_size("tm"), lax.axis_size("space"))
    role = lax.axis_index("tm") % 2
    side = lax.axis_index("space")
    scalars = jnp.stack([role, side]).astype(jnp.int32)
    shape = initial.shape[1:]
    depth = shape[0]
    initial, source = (initial[0], source[0])

    def number(t, s):
        return (t % tm) * space + s

    def permute(value, pairs):
        return lax.ppermute(value, ("tm", "space"), pairs)

    sides = range(space)
    stride, group = ROW, ROW * RUNS
    even, odd = range(0, tm, 2), range(1, tm, 2)
    into_odd = [(number(t, s), number(t + 1, s)) for t in even for s in sides]
    into_even = [(number(t, s), number(t + 1, s)) for t in odd for s in sides]
    short_even = [(number(t, s), number(t + 1, s)) for t in odd for s in sides if t % ROW < ROW - 1 or s == 0]
    last = [t for t in odd if t % ROW == ROW - 1]
    last_along = [(number(t, 1), number(t + 1 + CORES, 1)) for t in last]
    last_around = [(number(t + 1 + CORES, 1), number(t + 1, 1)) for t in last]
    across_even = [(number(t, s), number(t, 1 - s)) for t in even for s in sides]
    across_odd = [(number(t, s), number(t, 1 - s)) for t in odd for s in sides]
    odd_across = [(number(t, s), number(t + 1, 1 - s)) for t in even for s in sides]
    even_across = [(number(t, s), number(t + 1, 1 - s)) for t in odd for s in sides]
    lower_odd = []
    for t in odd:
        run, first = (t % group) // stride, t % stride == 1
        lower_odd.append((number(t, 1) if first else number(t - stride, 1) if run else number(t - 1, 1), number(t, 0)))
        if run < RUNS - 1:
            lower_odd.append((number(t + stride, 0), number(t, 1)))
        else:
            end = t % stride == stride - 1
            base = t - t % group
            lower_odd.append((number(base + HELPER if first else base + stride - CORES if end else t - 1, 0), number(t, 1)))
    back = [(number(t, s), number(t - 1, s)) for t in odd for s in sides]

    plane = shape[1:]
    ext = (depth + HALO,) + plane
    padded = (depth + HALO + 2,) + plane
    scratch = [pltpu.VMEM(padded, F32), pltpu.VMEM(padded, F32), pltpu.VMEM(ext, F32)]
    thin = (THIN,) + plane
    far = (initial, source, diffusion, advection)

    coef_edge, field_edge, thin_edge = call(
        pack_kernel, [(4 * ITERS,) + plane, (2 * ITERS,) + plane, thin], scalars, far=far, scratch=[pltpu.SemaphoreType.DMA((7,))]
    )
    si = permute(field_edge, across_even + across_odd)
    de = permute(thin_edge, even_across)
    b1 = permute(initial, into_even)
    sc = permute(coef_edge, lower_odd)
    *coefs, diag, source_near, full = call(
        own_kernel,
        [ext] * 5 + [shape] * 2 + [(depth + ITERS,) + plane],
        scalars,
        far=far,
        scratch=[pltpu.VMEM(shape, F32), pltpu.VMEM((3,) + shape, F32), pltpu.SemaphoreType.DMA((4,))],
    )
    (full,) = call(join_kernel, [(depth + ITERS,) + plane], scalars, si, full, aliases={2: 0})
    a1 = permute(full, into_odd)
    ac = permute(sc, back)

    def sweep(mine, others, v, vh, p, ph, p_halo, v_at=0, widths=(), extra=0, rims=()):
        nonlocal coefs
        outs = [shape] + [(w,) + plane for w in (1,) * extra + widths]
        kernel = functools.partial(sweep_kernel, mine, bool(others), widths, extra, len(p), v_at, p_halo, len(rims))
        operands = (*others, v, vh, source_near, si, *p, ph, *rims)
        made = [ext] * 5 if rims else []
        aliases = {1 + len(operands) + i: len(outs) + i for i in range(len(made))}
        out = call(kernel, outs + made, scalars, *operands, *coefs, scratch=scratch, aliases=aliases)
        if rims:
            out, coefs = out[:-5], out[-5:]
        return out

    x, xw, xt = sweep(1, (), full, full, (a1,), a1, (depth, ITERS), depth, (HALO, ITERS), rims=(sc,))
    b2 = permute(x, short_even)
    sx = permute(xw, across_odd)
    zh = permute(x, last_along)
    s1, yw = sweep(0, (), full, full, (b1,), de, (0, THIN), depth, (HALO,), rims=(ac,))
    dy = permute(yw, odd_across)
    a2 = permute(s1, into_odd)
    dx = permute(xt, even_across)
    yh = permute(zh, last_around)
    z, zh1 = sweep(1, (), x, sx, (a2,), dy, (0, HALO), extra=1)
    b3 = permute(z, into_even)
    ey = permute(dy, back)
    s2, s2h = sweep(0, (z, zh1), s1, ey, (b2, yh), dx, (0, ITERS), extra=1)
    a3 = permute(s2, into_odd)
    s2_far, defect = call(
        defect_kernel,
        [pltpu.HBM(shape, F32), shape],
        scalars,
        s2,
        s2h,
        source_near,
        *coefs[:4],
        diag,
        scratch=[pltpu.VMEM((depth + 2,) + plane, F32), pltpu.SemaphoreType.DMA],
    )
    (residual,) = call(
        add_kernel, [pltpu.HBM(shape, F32)], scalars, defect, a3, b3, scratch=[pltpu.VMEM(shape, F32), pltpu.SemaphoreType.DMA((2,))]
    )
    return (s2_far[None], residual[None])


def solution(mesh):
    in_specs = (
        P("tm", "space", None, None),
        P("tm", "space", None, None),
        P("space", None, None),
        P(None, "space", None, None),
    )
    out_specs = (P("tm", "space", None, None), P("tm", "space", None, None))
    return jax.shard_map(body, mesh=mesh, in_specs=in_specs, out_specs=out_specs, check_vma=False)
```
